32 devices in a mesh: dp: 2 (over z, core), ep: 16 (over x, y).
Axes of the slice: x: 4, y: 4, z: 1, core: 2. Of those that a mesh axis runs over, the one named last changes fastest.
The devices are a block of a 4x4x8 slice.
Arguments:
- x: bfloat16 [2, 16, 256, 2560], P('dp', 'ep'), parts along dimension 0
- expert: int32 [2, 16, 256, 8], P('dp', 'ep'), parts along dimension 0
- slot: int32 [2, 16, 256, 8], P('dp', 'ep'), parts along dimension 0
- gate: float32 [2, 16, 256, 8], P('dp', 'ep'), parts along dimension 0
- w_gate: bfloat16 [80, 2560, 1536], P('ep')
- w_up: bfloat16 [80, 2560, 1536], P('ep')
- w_down: bfloat16 [80, 1536, 2560], P('ep')
- s_gate: bfloat16 [2560, 1536], replicated
- s_up: bfloat16 [2560, 1536], replicated
- s_down: bfloat16 [1536, 2560], replicated
Outputs:
- y: bfloat16 [2, 16, 256, 2560], P('dp', 'ep'), parts along dimension 0
There are 2 independent parts. The reference program is written for one: setup_inputs(seed, part) draws one part's arguments, and reference() takes and returns one part's arrays. A program takes and returns all parts, laid end to end along the dimension named above; an argument that names none is the same for every part.
All inputs are finite; a program needn't handle non-finite values.
Results may differ from the reference program's by a relative error of at most 0.009.
Values are sent between devices in bfloat16 or wider.
A program may use at most 768 MiB of HBM per device.

```python
import jax
import jax.numpy as jnp

MEMBERS = 16
TOKENS = 256
D = 2560
FF = 1536
TOP = 8
EXPERTS = 80
SHARED_FF = 1536
SLOTS = 5 * TOKENS * TOP // (4 * EXPERTS)


def setup_inputs(seed: int = 0, part: int = 0) -> dict:
    own, k1, k2, k3, k4, k5, k6 = jax.random.split(jax.random.key(seed), 7)
    kx, ke, kl, kg = jax.random.split(jax.random.fold_in(own, part), 4)
    devices = (1, MEMBERS)
    place = jax.random.permutation(kl, jnp.arange(EXPERTS, dtype=jnp.uint32))
    slow = ((EXPERTS + (9 * place) % EXPERTS) << ((9 * place) // EXPERTS)) // EXPERTS
    wait = (jax.random.bits(ke, (*devices, TOKENS, EXPERTS), jnp.uint32) >> 10) * slow
    expert = jnp.argsort(wait, axis=-1)[..., :TOP].astype(jnp.int32)
    chosen = jax.nn.one_hot(expert, EXPERTS, dtype=jnp.int32)
    in_line = jnp.cumsum(chosen.reshape(*devices, TOKENS * TOP, EXPERTS), axis=2) - 1
    slot = jnp.sum(in_line.reshape(chosen.shape) * chosen, axis=-1)

    def one(key, rows, columns):
        return (jax.random.normal(key, (rows, columns), jnp.float32) * rows**-0.5).astype(jnp.bfloat16)

    def weights(key, rows, columns):
        return jax.lax.map(lambda k: one(k, rows, columns), jax.random.split(key, EXPERTS))

    return {
        "x": jax.random.normal(kx, (*devices, TOKENS, D), jnp.float32).astype(jnp.bfloat16),
        "expert": expert,
        "slot": slot,
        "gate": jax.nn.softmax(jax.random.normal(kg, expert.shape, jnp.float32)),
        "w_gate": weights(k1, D, FF),
        "w_up": weights(k2, D, FF),
        "w_down": weights(k3, FF, D),
        "s_gate": one(k4, D, SHARED_FF),
        "s_up": one(k5, D, SHARED_FF),
        "s_down": one(k6, SHARED_FF, D),
    }


def einsum(form, a, b):
    return jnp.einsum(form, a.astype(jnp.float32), b.astype(jnp.float32))


def for_all(x, s_gate, s_up, s_down):
    h = jax.nn.silu(einsum("...d,df->...f", x, s_gate)) * einsum("...d,df->...f", x, s_up)
    return einsum("...f,fd->...d", h.astype(jnp.bfloat16), s_down)


def reference(x, expert, slot, gate, w_gate, w_up, w_down, s_gate, s_up, s_down):
    to_expert = jax.nn.one_hot(expert, EXPERTS, dtype=jnp.bfloat16)
    to_slot = jax.nn.one_hot(slot, SLOTS, dtype=jnp.bfloat16)
    weighted = to_expert * gate[..., None].astype(jnp.bfloat16)
    dispatch = einsum("abtke,abtkc->abtec", to_expert, to_slot).astype(jnp.bfloat16)
    combine = einsum("abtke,abtkc->abtec", weighted, to_slot).astype(jnp.bfloat16)
    z = einsum("abtec,abtd->aebcd", dispatch, x).astype(jnp.bfloat16)
    h = jax.nn.silu(einsum("aebcd,edf->aebcf", z, w_gate))
    h = (h * einsum("aebcd,edf->aebcf", z, w_up)).astype(jnp.bfloat16)
    out = einsum("aebcf,efd->aebcd", h, w_down).astype(jnp.bfloat16)
    y = einsum("abtec,aebcd->abtd", combine, out)
    return (y + for_all(x, s_gate, s_up, s_down)).astype(jnp.bfloat16)
```

```python
import functools
import math

import jax
import jax.numpy as jnp
from jax import lax
from jax.experimental import pallas as pl
from jax.experimental.pallas import tpu as pltpu
from jax.sharding import PartitionSpec as P

MESH = pl.DeviceIdType.MESH
F32, BF16 = jnp.float32, jnp.bfloat16
VMEM_BYTES = 67_000_000
HALF = 256


def dot(a, b):
    return jnp.dot(a, b, preferred_element_type=F32)


class Place:
    def __init__(self, side):
        me = lax.axis_index("ep")
        self.side, self.x, self.y = side, me // side, me % side

    def at(self, dx, dy):
        s = self.side
        return (self.x + (dx % s)) % s * s + (self.y + (dy % s)) % s

    def first(self, half, d):
        return self.at(d, 0) if half == 0 else self.at(0, d)

    def second(self, half, d):
        return self.at(0, d) if half == 0 else self.at(d, 0)


def hits(rt, base, rows, tokens, weighted):
    row = lax.broadcasted_iota(jnp.int32, (rows, tokens), 0).astype(F32) + base.astype(F32)
    top = rt.shape[0] // 2
    total = jnp.zeros((rows, tokens), F32)
    for k in range(top):
        value = rt[top + k : top + k + 1, :] if weighted else jnp.ones((1, tokens), F32)
        total = total + jnp.where(rt[k : k + 1, :] == row, value, 0.0)
    return total


def expert_in(side, slots, chunks, rt_ref, x_ref, wg_hbm, wu_hbm, h_hbm, rt_out,
              rtb, raw, tran, pk, zb, dm, wgb, wub, accg, accu, ze, hst,
              rs, rr, ps, pr, ws, hs):
    place = Place(side)
    tokens, rows = x_ref.shape[0], dm.shape[3]
    experts, _, ff = accg.shape
    wide = 2 * HALF
    part = wgb.shape[2]
    parts = ff // part
    steps = chunks * experts * parts
    hops = range(1, side)

    barrier = pltpu.get_barrier_semaphore()
    for half in (0, 1):
        for d in hops:
            pl.semaphore_signal(barrier, inc=1, device_id={"ep": place.first(half, d)}, device_id_type=MESH)

    def weights(step):
        slot = step % 3
        c, e, n = step // (experts * parts), step // parts % experts, step % parts
        at = (e, pl.ds(pl.multiple_of(c * wide, wide), wide), pl.ds(pl.multiple_of(n * part, part), part))
        return (
            pltpu.make_async_copy(wg_hbm.at[at], wgb.at[slot], ws.at[0, slot]),
            pltpu.make_async_copy(wu_hbm.at[at], wub.at[slot], ws.at[1, slot]),
        )

    for step in (0, 1):
        for copy in weights(step):
            copy.start()
    for half in (0, 1):
        rtb[half, 0] = rt_ref[...]
    pl.semaphore_wait(barrier, 2 * (side - 1))

    def routing(half, d):
        return pltpu.make_async_remote_copy(
            src_ref=rt_ref, dst_ref=rtb.at[half, side - d], send_sem=rs.at[half, d], recv_sem=rr.at[half, side - d],
            device_id={"ep": place.first(half, d)}, device_id_type=MESH)

    def cols(half, c):
        return pl.ds(pl.multiple_of(c * wide + half * HALF, HALF), HALF)

    low, high = pl.ds(0, tokens // 2), pl.ds(tokens // 2, tokens // 2)

    def send(kind, half, c):
        plus, minus = (1, -1)
        src, dst, to = [
            lambda: (x_ref.at[:, cols(half, c)], raw.at[half, c, 2], place.first(half, plus)),
            lambda: (x_ref.at[:, cols(half, c)], raw.at[half, c, 0], place.first(half, minus)),
            lambda: (raw.at[half, c, 2, low], raw.at[half, c, 1, low], place.first(half, plus)),
            lambda: (raw.at[half, c, 0, high], raw.at[half, c, 1, high], place.first(half, minus)),
            lambda: (pk.at[half, 1, pl.ds(0, 2)], tran.at[half, c, 0], place.second(half, plus)),
            lambda: (pk.at[half, 1, pl.ds(2, 2)], tran.at[half, c, 1], place.second(half, minus)),
            lambda: (pk.at[half, 0], zb.at[half, c, 3], place.second(half, plus)),
            lambda: (pk.at[half, 2], zb.at[half, c, 1], place.second(half, minus)),
            lambda: (tran.at[half, c, 0], zb.at[half, c, 2, pl.ds(0, 2)], place.second(half, plus)),
            lambda: (tran.at[half, c, 1], zb.at[half, c, 2, pl.ds(2, 2)], place.second(half, minus)),
        ][kind]()
        return pltpu.make_async_remote_copy(
            src_ref=src, dst_ref=dst, send_sem=ps.at[kind, half, c], recv_sem=pr.at[kind, half, c],
            device_id={"ep": to}, device_id_type=MESH)

    def own_blocks(c):
        for half in (0, 1):
            send(0, half, c).start()
            send(1, half, c).start()

    def pass_blocks(c):
        for half in (0, 1):
            send(0, half, c).wait_recv()
            send(2, half, c).start()
            send(1, half, c).wait_recv()
            send(3, half, c).start()

    def pick(half, c, j):
        for r in range(side):
            block = x_ref[:, cols(half, c)] if r == 0 else raw[half, c, r - 1]
            rows_out = dot(dm[half, j, r], block).astype(BF16)
            if j == 0:
                zb[half, c, 0, r] = rows_out
            else:
                pk[half, j - 1, r] = rows_out

    def relay(c):
        for half in (0, 1):

            @pl.when(c > 0)
            def _():
                for kind in (4, 5, 6, 7):
                    send(kind, half, c - 1).wait_send()

            send(2, half, c).wait_recv()
            send(3, half, c).wait_recv()
            pick(half, c, 2)
            pick(half, c, 1)
            send(4, half, c).start()
            send(5, half, c).start()
            pick(half, c, 3)
            send(6, half, c).start()
            pick(half, c, 0)
            send(7, half, c).start()

    def pass_rows(c):
        for half in (0, 1):
            for kind in (4, 5):
                send(kind, half, c).wait_recv()
                send(kind + 4, half, c).start()

    def compute(c, last):
        for half in (0, 1):
            for kind in (6, 7, 8, 9):
                send(kind, half, c).wait_recv()

        def expert(e, carry):
            mine = pl.ds(pl.multiple_of(e * slots, slots), slots)
            for dx in range(side):
                for dy in range(side):
                    at = pl.ds((dx * side + dy) * slots, slots)
                    ze[at, 0:HALF] = zb[0, c, dy, dx, mine, :]
                    ze[at, HALF:wide] = zb[1, c, dx, dy, mine, :]
            for n in range(parts):
                step = (c * experts + e) * parts + n

                @pl.when(step + 2 < steps)
                def _():
                    for copy in weights(step + 2):
                        copy.start()

                for copy in weights(step):
                    copy.wait()
                slot = step % 3
                if last:

                    @pl.when(e > 0)
                    def _():
                        result(e - 1, n).wait()

                def tile(t, carry):
                    at = pl.ds(pl.multiple_of(t * 256, 256), 256)
                    to = pl.ds(pl.multiple_of(n * part + t * 256, 256), 256)
                    g = accg[e, :, to] + dot(ze[...], wgb[slot, :, at])
                    u = accu[e, :, to] + dot(ze[...], wub[slot, :, at])
                    if last:
                        hst[n, :, at] = (jax.nn.silu(g) * u).astype(BF16)
                    else:
                        accg[e, :, to] = g
                        accu[e, :, to] = u
                    return carry

                lax.fori_loop(0, part // 256, tile, 0)
                if last:
                    result(e, n).start()
            return carry

        lax.fori_loop(0, experts, expert, 0)

    def result(e, n):
        return pltpu.make_async_copy(hst.at[n], h_hbm.at[e, :, pl.ds(n * part, part)], hs.at[n])

    own_blocks(0)
    for half in (0, 1):
        for d in hops:
            routing(half, d).start()
    own_blocks(1)

    def clear(i, carry):
        at = pl.ds(pl.multiple_of(i * 128, 128), 128)
        for e in range(experts):
            accg[e, :, at] = jnp.zeros((accg.shape[1], 128), F32)
            accu[e, :, at] = jnp.zeros((accg.shape[1], 128), F32)
        return carry

    pass_blocks(0)
    lax.fori_loop(0, ff // 128, clear, 0)
    for half in (0, 1):
        for d in hops:
            routing(half, d).wait_recv()
        for r in range(side):
            for j in range(side):
                base = place.second(half, j) * rows
                dm[half, j, r] = hits(rtb[half, r], base, rows, tokens, False).astype(BF16)
    relay(0)
    pass_blocks(1)
    own_blocks(2)

    def chunk(c, carry):
        pass_rows(c)
        relay(c + 1)

        @pl.when(c + 2 < chunks)
        def _():
            pass_blocks(c + 2)

        @pl.when(c + 3 < chunks)
        def _():
            own_blocks(c + 3)

        compute(c, False)
        return carry

    lax.fori_loop(0, chunks - 1, chunk, 0)
    pass_rows(chunks - 1)
    compute(chunks - 1, True)
    for n in range(parts):
        result(experts - 1, n).wait()
    rt_out[...] = rtb[...]

    def drain(c, carry):
        for half in (0, 1):
            for kind in (0, 1, 2, 3, 8, 9):
                send(kind, half, c).wait_send()
        return carry

    lax.fori_loop(0, chunks, drain, 0)
    for half in (0, 1):
        for kind in (4, 5, 6, 7):
            send(kind, half, chunks - 1).wait_send()
        for d in hops:
            routing(half, d).wait_send()


def expert_out(side, slots, chunks, rt_ref, x_ref, h_hbm, wd_hbm, sg_hbm, su_hbm, sd_hbm, y_ref,
               hb, wdb, ob, rb, tran, cm, summed, hs, hr, ss, sr, yacc, sgb, sub, sdb, hsb,
               ps, pr, ws, hsem, ssem):
    place = Place(side)
    tokens = x_ref.shape[0]
    rows = ob.shape[4]
    experts = hb.shape[0]
    ff = hsb.shape[1]
    wide = 2 * HALF
    steps = chunks * experts
    half_rows = tokens // 2
    low, high = pl.ds(0, half_rows), pl.ds(half_rows, half_rows)

    barrier = pltpu.get_barrier_semaphore()
    for half in (0, 1):
        for d in (1, -1):
            pl.semaphore_signal(barrier, inc=1, device_id={"ep": place.first(half, d)}, device_id_type=MESH)

    def load_h(e):
        return pltpu.make_async_copy(h_hbm.at[e], hb.at[e], hsem.at[e])

    def weights(step):
        slot = step % 2
        c, e = step // experts, step % experts
        return pltpu.make_async_copy(
            wd_hbm.at[e, :, pl.ds(pl.multiple_of(c * wide, wide), wide)], wdb.at[slot], ws.at[slot])

    load_h(0).start()
    weights(0).start()
    for e in range(1, experts):
        load_h(e).start()

    def send(kind, half, c):
        plus, minus = (1, -1)
        par = c % 2
        src, dst, to = [
            lambda: (ob.at[half, par, 2, pl.ds(0, 2)], tran.at[half, c, 0], place.second(half, plus)),
            lambda: (ob.at[half, par, 2, pl.ds(2, 2)], tran.at[half, c, 1], place.second(half, minus)),
            lambda: (ob.at[half, par, 1], rb.at[half, c, 2], place.second(half, plus)),
            lambda: (ob.at[half, par, 3], rb.at[half, c, 0], place.second(half, minus)),
            lambda: (tran.at[half, c, 0], rb.at[half, c, 1, pl.ds(0, 2)], place.second(half, plus)),
            lambda: (tran.at[half, c, 1], rb.at[half, c, 1, pl.ds(2, 2)], place.second(half, minus)),
            lambda: (hs.at[half, 0], hr.at[half, c, 0], place.first(half, plus)),
            lambda: (hs.at[half, 1], hr.at[half, c, 1], place.first(half, minus)),
            lambda: (ss.at[half, 0], sr.at[half, c, 0], place.first(half, plus)),
            lambda: (ss.at[half, 1], sr.at[half, c, 1], place.first(half, minus)),
        ][kind]()
        return pltpu.make_async_remote_copy(
            src_ref=src, dst_ref=dst, send_sem=ps.at[kind, half, c], recv_sem=pr.at[kind, half, c],
            device_id={"ep": to}, device_id_type=MESH)

    def down(c):
        par = c % 2

        def expert(e, carry):
            step = c * experts + e

            @pl.when(step + 1 < steps)
            def _():
                weights(step + 1).start()

            weights(step).wait()
            mine = pl.ds(pl.multiple_of(e * slots, slots), slots)
            for half in (0, 1):
                out = dot(hb[e], wdb[step % 2, :, half * HALF : (half + 1) * HALF]).astype(BF16)
                for dx in range(side):
                    for dy in range(side):
                        j, r = (dy, dx) if half == 0 else (dx, dy)
                        at = (dx * side + dy) * slots
                        ob[half, par, j, r, mine, :] = out[at : at + slots]
            return carry

        lax.fori_loop(0, experts, expert, 0)

    def send_rows(c):
        for half in (0, 1):
            for kind in (0, 1, 2, 3):
                send(kind, half, c).start()

    def pass_rows(c):
        for half in (0, 1):
            for kind in (0, 1):
                send(kind, half, c).wait_recv()
                send(kind + 4, half, c).start()

    def relay(c):
        par = c % 2
        for half in (0, 1):
            for kind in (2, 3, 4, 5):
                send(kind, half, c).wait_recv()

            def total(r):
                out = dot(cm[half, 0, r], ob[half, par, 0, r])
                for j in range(1, side):
                    out = out + dot(cm[half, j, r], rb[half, c, j - 1, r])
                return out

            far = total(2).astype(BF16)

            @pl.when(c > 0)
            def _():
                for kind in (6, 7):
                    send(kind, half, c - 1).wait_send()

            hs[half, 0] = far[:half_rows]
            hs[half, 1] = far[half_rows:]
            summed[half, 0] = total(1)
            send(6, half, c).start()
            summed[half, 1] = total(3)
            send(7, half, c).start()
            at = pl.ds(pl.multiple_of(c * wide + half * HALF, HALF), HALF)
            yacc[:, at] += total(0)

    def near(c):
        for half in (0, 1):

            @pl.when(c > 0)
            def _():
                for kind in (8, 9):
                    send(kind, half, c - 1).wait_send()

            send(6, half, c).wait_recv()
            ss[half, 0, low] = (summed[half, 0, low] + hr[half, c, 0].astype(F32)).astype(BF16)
            ss[half, 0, high] = summed[half, 0, high].astype(BF16)
            send(7, half, c).wait_recv()
            ss[half, 1, low] = summed[half, 1, low].astype(BF16)
            ss[half, 1, high] = (summed[half, 1, high] + hr[half, c, 1].astype(F32)).astype(BF16)
            send(8, half, c).start()
            send(9, half, c).start()

    def finish(c):
        for half in (0, 1):
            for kind in (8, 9):
                send(kind, half, c).wait_recv()
            at = pl.ds(pl.multiple_of(c * wide + half * HALF, HALF), HALF)
            total = yacc[:, at] + sr[half, c, 0].astype(F32) + sr[half, c, 1].astype(F32)
            y_ref[:, at] = total.astype(BF16)

    def shared_in(n):
        at = pl.ds(pl.multiple_of(n * 256, 256), 256)
        return (
            pltpu.make_async_copy(sg_hbm.at[:, at], sgb.at[n % 2], ssem.at[0, n % 2]),
            pltpu.make_async_copy(su_hbm.at[:, at], sub.at[n % 2], ssem.at[1, n % 2]),
        )

    def shared_out(n):
        at = pl.ds(pl.multiple_of(n * wide, wide), wide)
        return pltpu.make_async_copy(sd_hbm.at[:, at], sdb.at[n % 2], ssem.at[2, n % 2])

    def shared():
        def inner(n, carry):
            @pl.when(n + 1 < ff // 256)
            def _():
                for copy in shared_in(n + 1):
                    copy.start()

            for copy in shared_in(n):
                copy.wait()
            g = dot(x_ref[...], sgb[n % 2])
            u = dot(x_ref[...], sub[n % 2])
            hsb[:, pl.ds(pl.multiple_of(n * 256, 256), 256)] = (jax.nn.silu(g) * u).astype(BF16)
            return carry

        lax.fori_loop(0, ff // 256, inner, 0)

        def outer(n, carry):
            @pl.when(n + 1 < chunks)
            def _():
                shared_out(n + 1).start()

            shared_out(n).wait()
            yacc[:, pl.ds(pl.multiple_of(n * wide, wide), wide)] = dot(hsb[...], sdb[n % 2])
            return carry

        lax.fori_loop(0, chunks, outer, 0)

    for e in range(experts):
        load_h(e).wait()
    down(0)
    pl.semaphore_wait(barrier, 4)
    send_rows(0)
    for copy in shared_in(0):
        copy.start()
    shared_out(0).start()
    for half in (0, 1):
        for r in range(side):
            for j in range(side):
                base = place.second(half, j) * rows
                cm[half, j, r] = hits(rt_ref[half, r], base, rows, tokens, True).T.astype(BF16)
    pass_rows(0)
    down(1)
    send_rows(1)
    shared()

    def chunk(c, carry):
        @pl.when(c > 0)
        def _():
            near(c - 1)

        relay(c)

        @pl.when(c + 1 < chunks)
        def _():
            pass_rows(c + 1)

        @pl.when(c + 2 < chunks)
        def _():
            for half in (0, 1):
                for kind in (0, 1, 2, 3):
                    send(kind, half, c).wait_send()
            down(c + 2)
            send_rows(c + 2)

        @pl.when(c > 1)
        def _():
            finish(c - 2)

        return carry

    lax.fori_loop(0, chunks, chunk, 0)
    near(chunks - 1)
    finish(chunks - 2)
    finish(chunks - 1)

    for half in (0, 1):
        for kind in (6, 7, 8, 9):
            send(kind, half, chunks - 1).wait_send()
        for c in (chunks - 2, chunks - 1):
            for kind in (0, 1, 2, 3):
                send(kind, half, c).wait_send()

    def drain(c, carry):
        for half in (0, 1):
            for kind in (4, 5):
                send(kind, half, c).wait_send()
        return carry

    lax.fori_loop(0, chunks, drain, 0)


def solution(mesh):
    members = mesh.shape["ep"]
    side = math.isqrt(members)

    def local(x, expert, slot, gate, w_gate, w_up, w_down, s_gate, s_up, s_down):
        x, expert, slot, gate = x[0, 0], expert[0, 0], slot[0, 0], gate[0, 0]
        (tokens, top), (experts, d, ff) = expert.shape, w_gate.shape
        slots = 5 * tokens * top // (4 * experts * members)
        rows, wide = experts * slots, 2 * HALF
        chunks = d // wide
        part = ff // 2
        key = jnp.where(slot < slots, expert * slots + slot, -1).astype(F32)
        weight = gate.astype(BF16).astype(F32)
        rt = jnp.concatenate([key.T, weight.T], axis=0)

        vmem, anywhere = pl.BlockSpec(memory_space=pltpu.VMEM), pl.BlockSpec(memory_space=pl.ANY)
        dma = pltpu.SemaphoreType.DMA

        def buf(*shape, dtype=BF16):
            return pltpu.VMEM(shape, dtype)

        h, rt_all = pl.pallas_call(
            functools.partial(expert_in, side, slots, chunks),
            out_shape=(
                jax.ShapeDtypeStruct((experts, members * slots, ff), BF16),
                jax.ShapeDtypeStruct((2, side, 2 * top, tokens), F32),
            ),
            in_specs=[vmem, vmem, anywhere, anywhere],
            out_specs=(anywhere, vmem),
            scratch_shapes=[
                buf(2, side, 2 * top, tokens, dtype=F32),
                buf(2, chunks, 3, tokens, HALF),
                buf(2, chunks, 2, 2, rows, HALF),
                buf(2, 3, side, rows, HALF),
                buf(2, chunks, side, side, rows, HALF),
                buf(2, side, side, rows, tokens),
                buf(3, wide, part),
                buf(3, wide, part),
                buf(experts, members * slots, ff, dtype=F32),
                buf(experts, members * slots, ff, dtype=F32),
                buf(members * slots, wide),
                buf(2, members * slots, part),
                dma((2, side)),
                dma((2, side)),
                dma((10, 2, chunks)),
                dma((10, 2, chunks)),
                dma((2, 3)),
                dma((2,)),
            ],
            compiler_params=pltpu.CompilerParams(collective_id=0, has_side_effects=True, vmem_limit_bytes=VMEM_BYTES),
            name="expert_in",
        )(rt, x, w_gate, w_up)

        y = pl.pallas_call(
            functools.partial(expert_out, side, slots, chunks),
            out_shape=jax.ShapeDtypeStruct((tokens, d), BF16),
            in_specs=[vmem, vmem] + [anywhere] * 5,
            out_specs=vmem,
            scratch_shapes=[
                buf(experts, members * slots, ff),
                buf(2, ff, wide),
                buf(2, 2, side, side, rows, HALF),
                buf(2, chunks, 3, side, rows, HALF),
                buf(2, chunks, 2, 2, rows, HALF),
                buf(2, side, side, tokens, rows),
                buf(2, 2, tokens, HALF, dtype=F32),
                buf(2, 2, tokens // 2, HALF),
                buf(2, chunks, 2, tokens // 2, HALF),
                buf(2, 2, tokens, HALF),
                buf(2, chunks, 2, tokens, HALF),
                buf(tokens, d, dtype=F32),
                buf(2, d, 256),
                buf(2, d, 256),
                buf(2, ff, wide),
                buf(tokens, ff),
                dma((10, 2, chunks)),
                dma((10, 2, chunks)),
                dma((2,)),
                dma((experts,)),
                dma((3, 2)),
            ],
            compiler_params=pltpu.CompilerParams(collective_id=1, has_side_effects=True, vmem_limit_bytes=VMEM_BYTES),
            name="expert_out",
        )(rt_all, x, h, w_down, s_gate, s_up, s_down)
        return y[None, None]

    tok = P("dp", "ep", None, None)
    return jax.shard_map(
        local,
        mesh=mesh,
        in_specs=(tok, tok, tok, tok, P("ep"), P("ep"), P("ep"), P(), P(), P()),
        out_specs=tok,
        check_vma=False,
    )
```

```python
import functools
import math

import jax
import jax.numpy as jnp
from jax import lax
from jax.experimental import pallas as pl
from jax.experimental.pallas import tpu as pltpu
from jax.sharding import PartitionSpec as P

MESH = pl.DeviceIdType.MESH
F32, BF16 = jnp.float32, jnp.bfloat16
VMEM_BYTES = 67_000_000
HALF = 256


def dot(a, b):
    return jnp.dot(a, b, preferred_element_type=F32)


class Place:
    def __init__(self, side):
        me = lax.axis_index("ep")
        self.side, self.x, self.y = side, me // side, me % side

    def at(self, dx, dy):
        s = self.side
        return (self.x + (dx % s)) % s * s + (self.y + (dy % s)) % s

    def first(self, half, d):
        return self.at(d, 0) if half == 0 else self.at(0, d)

    def second(self, half, d):
        return self.at(0, d) if half == 0 else self.at(d, 0)


def hits(rt, base, rows, tokens, weighted):
    row = lax.broadcasted_iota(jnp.int32, (rows, tokens), 0).astype(F32) + base.astype(F32)
    top = rt.shape[0] // 2
    total = jnp.zeros((rows, tokens), F32)
    for k in range(top):
        value = rt[top + k : top + k + 1, :] if weighted else jnp.ones((1, tokens), F32)
        total = total + jnp.where(rt[k : k + 1, :] == row, value, 0.0)
    return total


def expert_in(side, slots, chunks, rt_ref, x_ref, wg_hbm, wu_hbm, h_hbm, rt_out,
              rtb, raw, tran, pk, zb, dm, wgb, wub, accg, accu, ze, hst,
              rs, rr, ps, pr, ws, hs):
    place = Place(side)
    tokens, rows = x_ref.shape[0], dm.shape[3]
    experts, _, ff = accg.shape
    wide = 2 * HALF
    part = wgb.shape[2]
    parts = ff // part
    steps = chunks * experts * parts
    hops = range(1, side)

    barrier = pltpu.get_barrier_semaphore()
    for half in (0, 1):
        for d in hops:
            pl.semaphore_signal(barrier, inc=1, device_id={"ep": place.first(half, d)}, device_id_type=MESH)

    def weights(step):
        slot = step % 3
        c, e, n = step // (experts * parts), step // parts % experts, step % parts
        at = (e, pl.ds(pl.multiple_of(c * wide, wide), wide), pl.ds(pl.multiple_of(n * part, part), part))
        return (
            pltpu.make_async_copy(wg_hbm.at[at], wgb.at[slot], ws.at[0, slot]),
            pltpu.make_async_copy(wu_hbm.at[at], wub.at[slot], ws.at[1, slot]),
        )

    for step in (0, 1):
        for copy in weights(step):
            copy.start()
    for half in (0, 1):
        rtb[half, 0] = rt_ref[...]
    pl.semaphore_wait(barrier, 2 * (side - 1))

    def routing(half, d):
        return pltpu.make_async_remote_copy(
            src_ref=rt_ref, dst_ref=rtb.at[half, side - d], send_sem=rs.at[half, d], recv_sem=rr.at[half, side - d],
            device_id={"ep": place.first(half, d)}, device_id_type=MESH)

    def cols(half, c):
        return pl.ds(pl.multiple_of(c * wide + half * HALF, HALF), HALF)

    low, high = pl.ds(0, tokens // 2), pl.ds(tokens // 2, tokens // 2)

    def send(kind, half, c):
        plus, minus = (1, -1)
        src, dst, to = [
            lambda: (x_ref.at[:, cols(half, c)], raw.at[half, c, 2], place.first(half, plus)),
            lambda: (x_ref.at[:, cols(half, c)], raw.at[half, c, 0], place.first(half, minus)),
            lambda: (raw.at[half, c, 2, low], raw.at[half, c, 1, low], place.first(half, plus)),
            lambda: (raw.at[half, c, 0, high], raw.at[half, c, 1, high], place.first(half, minus)),
            lambda: (pk.at[half, 1, pl.ds(0, 2)], tran.at[half, c, 0], place.second(half, plus)),
            lambda: (pk.at[half, 1, pl.ds(2, 2)], tran.at[half, c, 1], place.second(half, minus)),
            lambda: (pk.at[half, 0], zb.at[half, c, 3], place.second(half, plus)),
            lambda: (pk.at[half, 2], zb.at[half, c, 1], place.second(half, minus)),
            lambda: (tran.at[half, c, 0], zb.at[half, c, 2, pl.ds(0, 2)], place.second(half, plus)),
            lambda: (tran.at[half, c, 1], zb.at[half, c, 2, pl.ds(2, 2)], place.second(half, minus)),
        ][kind]()
        return pltpu.make_async_remote_copy(
            src_ref=src, dst_ref=dst, send_sem=ps.at[kind, half, c], recv_sem=pr.at[kind, half, c],
            device_id={"ep": to}, device_id_type=MESH)

    def own_blocks(c):
        for half in (0, 1):
            send(0, half, c).start()
            send(1, half, c).start()

    def pass_blocks(c):
        for half in (0, 1):
            send(0, half, c).wait_recv()
            send(2, half, c).start()
            send(1, half, c).wait_recv()
            send(3, half, c).start()

    def pick(half, c, j):
        for r in range(side):
            block = x_ref[:, cols(half, c)] if r == 0 else raw[half, c, r - 1]
            rows_out = dot(dm[half, j, r], block).astype(BF16)
            if j == 0:
                zb[half, c, 0, r] = rows_out
            else:
                pk[half, j - 1, r] = rows_out

    def relay(half, c):
        @pl.when(c > 0)
        def _():
            for kind in (4, 5, 6, 7):
                send(kind, half, c - 1).wait_send()

        send(2, half, c).wait_recv()
        send(3, half, c).wait_recv()
        pick(half, c, 2)
        pick(half, c, 1)
        send(4, half, c).start()
        send(5, half, c).start()
        pick(half, c, 3)
        send(6, half, c).start()
        pick(half, c, 0)
        send(7, half, c).start()

    def pass_rows(c):
        for half in (0, 1):
            for kind in (4, 5):
                send(kind, half, c).wait_recv()
                send(kind + 4, half, c).start()

    def arrive(c):
        for half in (0, 1):
            for kind in (6, 7, 8, 9):
                send(kind, half, c).wait_recv()

    def compute(c, first, end, last):
        def expert(e, carry):
            mine = pl.ds(pl.multiple_of(e * slots, slots), slots)
            for dx in range(side):
                for dy in range(side):
                    at = pl.ds((dx * side + dy) * slots, slots)
                    ze[at, 0:HALF] = zb[0, c, dy, dx, mine, :]
                    ze[at, HALF:wide] = zb[1, c, dx, dy, mine, :]

            def columns(n, carry):
                step = (c * experts + e) * parts + n

                @pl.when(step + 2 < steps)
                def _():
                    for copy in weights(step + 2):
                        copy.start()

                for copy in weights(step):
                    copy.wait()
                slot = step % 3
                if last:

                    @pl.when(e > 0)
                    def _():
                        result(e - 1, n).wait()

                for t in range(part // 256):
                    at = pl.ds(t * 256, 256)
                    to = pl.ds(pl.multiple_of(n * part + t * 256, 256), 256)
                    g = accg[e, :, to] + dot(ze[...], wgb[slot, :, at])
                    u = accu[e, :, to] + dot(ze[...], wub[slot, :, at])
                    if last:
                        hst[n, :, at] = (jax.nn.silu(g) * u).astype(BF16)
                    else:
                        accg[e, :, to] = g
                        accu[e, :, to] = u
                if last:
                    result(e, n).start()
                return carry

            return lax.fori_loop(0, parts, columns, carry)

        lax.fori_loop(first, end, expert, 0)

    def result(e, n):
        return pltpu.make_async_copy(hst.at[n], h_hbm.at[e, :, pl.ds(pl.multiple_of(n * part, part), part)], hs.at[n])

    own_blocks(0)
    for half in (0, 1):
        for d in hops:
            routing(half, d).start()
    own_blocks(1)

    def clear(i, carry):
        at = pl.ds(pl.multiple_of(i * 128, 128), 128)
        for e in range(experts):
            accg[e, :, at] = jnp.zeros((accg.shape[1], 128), F32)
            accu[e, :, at] = jnp.zeros((accg.shape[1], 128), F32)
        return carry

    pass_blocks(0)
    lax.fori_loop(0, ff // 128, clear, 0)
    for half in (0, 1):
        for d in hops:
            routing(half, d).wait_recv()
        for r in range(side):
            for j in range(side):
                base = place.second(half, j) * rows
                dm[half, j, r] = hits(rtb[half, r], base, rows, tokens, False).astype(BF16)
    relay(0, 0)
    relay(1, 0)
    pass_blocks(1)
    own_blocks(2)

    def chunk(c, carry):
        pass_rows(c)

        @pl.when(c + 1 < chunks)
        def _():
            relay(0, c + 1)

        @pl.when(c > 0)
        def _():
            arrive(c - 1)
            compute(c - 1, 0, 2, False)

        @pl.when(c + 1 < chunks)
        def _():
            relay(1, c + 1)

        @pl.when(c > 0)
        def _():
            compute(c - 1, 2, 3, False)

        @pl.when(c + 2 < chunks)
        def _():
            pass_blocks(c + 2)

        @pl.when(c > 0)
        def _():
            compute(c - 1, 3, experts, False)

        @pl.when(c + 3 < chunks)
        def _():
            own_blocks(c + 3)

        return carry

    lax.fori_loop(0, chunks, chunk, 0)
    arrive(chunks - 1)
    compute(chunks - 1, 0, experts, True)
    for n in range(parts):
        result(experts - 1, n).wait()
    rt_out[...] = rtb[...]

    def drain(c, carry):
        for half in (0, 1):
            for kind in (0, 1, 2, 3, 8, 9):
                send(kind, half, c).wait_send()
        return carry

    lax.fori_loop(0, chunks, drain, 0)
    for half in (0, 1):
        for kind in (4, 5, 6, 7):
            send(kind, half, chunks - 1).wait_send()
        for d in hops:
            routing(half, d).wait_send()


def expert_out(side, slots, chunks, rt_ref, x_ref, h_hbm, wd_hbm, sg_hbm, su_hbm, sd_hbm, y_ref,
               hb, wdb, ob, rb, tran, cm, summed, hs, hr, ss, sr, yacc, sgb, sub, sdb, hsb,
               ps, pr, ws, hsem, ssem):
    place = Place(side)
    tokens = x_ref.shape[0]
    rows = ob.shape[4]
    experts = hb.shape[0]
    ff = hsb.shape[1]
    wide = 2 * HALF
    steps = chunks * experts
    half_rows = tokens // 2
    low, high = pl.ds(0, half_rows), pl.ds(half_rows, half_rows)

    barrier = pltpu.get_barrier_semaphore()
    for half in (0, 1):
        for d in (1, -1):
            pl.semaphore_signal(barrier, inc=1, device_id={"ep": place.first(half, d)}, device_id_type=MESH)

    def load_h(e):
        return pltpu.make_async_copy(h_hbm.at[e], hb.at[e], hsem.at[e])

    def weights(step):
        slot = step % 2
        c, e = step // experts, step % experts
        return pltpu.make_async_copy(
            wd_hbm.at[e, :, pl.ds(pl.multiple_of(c * wide, wide), wide)], wdb.at[slot], ws.at[slot])

    load_h(0).start()
    weights(0).start()
    for e in range(1, experts):
        load_h(e).start()

    def send(kind, half, c):
        plus, minus = (1, -1)
        par = c % 2
        src, dst, to = [
            lambda: (ob.at[half, par, 2, pl.ds(0, 2)], tran.at[half, c, 0], place.second(half, plus)),
            lambda: (ob.at[half, par, 2, pl.ds(2, 2)], tran.at[half, c, 1], place.second(half, minus)),
            lambda: (ob.at[half, par, 1], rb.at[half, c, 2], place.second(half, plus)),
            lambda: (ob.at[half, par, 3], rb.at[half, c, 0], place.second(half, minus)),
            lambda: (tran.at[half, c, 0], rb.at[half, c, 1, pl.ds(0, 2)], place.second(half, plus)),
            lambda: (tran.at[half, c, 1], rb.at[half, c, 1, pl.ds(2, 2)], place.second(half, minus)),
            lambda: (hs.at[half, 0], hr.at[half, c, 0], place.first(half, plus)),
            lambda: (hs.at[half, 1], hr.at[half, c, 1], place.first(half, minus)),
            lambda: (ss.at[half, 0], sr.at[half, c, 0], place.first(half, plus)),
            lambda: (ss.at[half, 1], sr.at[half, c, 1], place.first(half, minus)),
        ][kind]()
        return pltpu.make_async_remote_copy(
            src_ref=src, dst_ref=dst, send_sem=ps.at[kind, half, c], recv_sem=pr.at[kind, half, c],
            device_id={"ep": to}, device_id_type=MESH)

    def down(c, loading=False):
        par = c % 2

        def expert(e, carry):
            step = c * experts + e

            @pl.when(step + 1 < steps)
            def _():
                weights(step + 1).start()

            weights(step).wait()
            if loading:
                load_h(e).wait()
            mine = pl.ds(pl.multiple_of(e * slots, slots), slots)
            for half in (0, 1):
                out = dot(hb[e], wdb[step % 2, :, half * HALF : (half + 1) * HALF]).astype(BF16)
                for dx in range(side):
                    for dy in range(side):
                        j, r = (dy, dx) if half == 0 else (dx, dy)
                        at = (dx * side + dy) * slots
                        ob[half, par, j, r, mine, :] = out[at : at + slots]
            return carry

        lax.fori_loop(0, experts, expert, 0)

    def send_rows(c):
        for half in (0, 1):
            for kind in (0, 1, 2, 3):
                send(kind, half, c).start()

    def pass_rows(c):
        for half in (0, 1):
            for kind in (0, 1):
                send(kind, half, c).wait_recv()
                send(kind + 4, half, c).start()

    def relay(c):
        par = c % 2
        for half in (0, 1):
            for kind in (2, 3, 4, 5):
                send(kind, half, c).wait_recv()

            def total(r):
                out = dot(cm[half, 0, r], ob[half, par, 0, r])
                for j in range(1, side):
                    out = out + dot(cm[half, j, r], rb[half, c, j - 1, r])
                return out

            far = total(2).astype(BF16)

            @pl.when(c > 0)
            def _():
                for kind in (6, 7):
                    send(kind, half, c - 1).wait_send()

            hs[half, 0] = far[:half_rows]
            hs[half, 1] = far[half_rows:]
            summed[half, 0] = total(1)
            send(6, half, c).start()
            summed[half, 1] = total(3)
            send(7, half, c).start()
            at = pl.ds(pl.multiple_of(c * wide + half * HALF, HALF), HALF)
            yacc[:, at] += total(0)

    def near(c):
        for half in (0, 1):

            @pl.when(c > 0)
            def _():
                for kind in (8, 9):
                    send(kind, half, c - 1).wait_send()

            send(6, half, c).wait_recv()
            ss[half, 0, low] = (summed[half, 0, low] + hr[half, c, 0].astype(F32)).astype(BF16)
            ss[half, 0, high] = summed[half, 0, high].astype(BF16)
            send(7, half, c).wait_recv()
            ss[half, 1, low] = summed[half, 1, low].astype(BF16)
            ss[half, 1, high] = (summed[half, 1, high] + hr[half, c, 1].astype(F32)).astype(BF16)
            send(8, half, c).start()
            send(9, half, c).start()

    def finish(c):
        for half in (0, 1):
            for kind in (8, 9):
                send(kind, half, c).wait_recv()
            at = pl.ds(pl.multiple_of(c * wide + half * HALF, HALF), HALF)
            total = yacc[:, at] + sr[half, c, 0].astype(F32) + sr[half, c, 1].astype(F32)
            y_ref[:, at] = total.astype(BF16)

    def shared_in(n):
        at = pl.ds(pl.multiple_of(n * 256, 256), 256)
        return (
            pltpu.make_async_copy(sg_hbm.at[:, at], sgb.at[n % 2], ssem.at[0, n % 2]),
            pltpu.make_async_copy(su_hbm.at[:, at], sub.at[n % 2], ssem.at[1, n % 2]),
        )

    def shared_out(n):
        at = pl.ds(pl.multiple_of(n * wide, wide), wide)
        return pltpu.make_async_copy(sd_hbm.at[:, at], sdb.at[n % 2], ssem.at[2, n % 2])

    def shared():
        def inner(n, carry):
            @pl.when(n + 1 < ff // 256)
            def _():
                for copy in shared_in(n + 1):
                    copy.start()

            for copy in shared_in(n):
                copy.wait()
            g = dot(x_ref[...], sgb[n % 2])
            u = dot(x_ref[...], sub[n % 2])
            hsb[:, pl.ds(pl.multiple_of(n * 256, 256), 256)] = (jax.nn.silu(g) * u).astype(BF16)
            return carry

        lax.fori_loop(0, ff // 256, inner, 0)

        def outer(n, carry):
            @pl.when(n + 1 < chunks)
            def _():
                shared_out(n + 1).start()

            shared_out(n).wait()
            yacc[:, pl.ds(pl.multiple_of(n * wide, wide), wide)] = dot(hsb[...], sdb[n % 2])
            return carry

        lax.fori_loop(0, chunks, outer, 0)

    down(0, True)
    pl.semaphore_wait(barrier, 4)
    send_rows(0)
    for copy in shared_in(0):
        copy.start()
    shared_out(0).start()
    for half in (0, 1):
        for r in range(side):
            for j in range(side):
                base = place.second(half, j) * rows
                cm[half, j, r] = hits(rt_ref[half, r], base, rows, tokens, True).T.astype(BF16)
    pass_rows(0)
    down(1)
    send_rows(1)
    shared()

    def chunk(c, carry):
        @pl.when(c > 0)
        def _():
            near(c - 1)

        relay(c)

        @pl.when(c + 1 < chunks)
        def _():
            pass_rows(c + 1)

        @pl.when(c + 2 < chunks)
        def _():
            for half in (0, 1):
                for kind in (0, 1, 2, 3):
                    send(kind, half, c).wait_send()
            down(c + 2)
            send_rows(c + 2)

        @pl.when(c > 1)
        def _():
            finish(c - 2)

        return carry

    lax.fori_loop(0, chunks, chunk, 0)
    near(chunks - 1)
    finish(chunks - 2)
    finish(chunks - 1)

    for half in (0, 1):
        for kind in (6, 7, 8, 9):
            send(kind, half, chunks - 1).wait_send()
        for c in (chunks - 2, chunks - 1):
            for kind in (0, 1, 2, 3):
                send(kind, half, c).wait_send()

    def drain(c, carry):
        for half in (0, 1):
            for kind in (4, 5):
                send(kind, half, c).wait_send()
        return carry

    lax.fori_loop(0, chunks, drain, 0)


def solution(mesh):
    members = mesh.shape["ep"]
    side = math.isqrt(members)

    def local(x, expert, slot, gate, w_gate, w_up, w_down, s_gate, s_up, s_down):
        x, expert, slot, gate = x[0, 0], expert[0, 0], slot[0, 0], gate[0, 0]
        (tokens, top), (experts, d, ff) = expert.shape, w_gate.shape
        slots = 5 * tokens * top // (4 * experts * members)
        rows, wide = experts * slots, 2 * HALF
        chunks = d // wide
        part = ff // 2
        key = jnp.where(slot < slots, expert * slots + slot, -1).astype(F32)
        weight = gate.astype(BF16).astype(F32)
        rt = jnp.concatenate([key.T, weight.T], axis=0)

        vmem, anywhere = pl.BlockSpec(memory_space=pltpu.VMEM), pl.BlockSpec(memory_space=pl.ANY)
        dma = pltpu.SemaphoreType.DMA

        def buf(*shape, dtype=BF16):
            return pltpu.VMEM(shape, dtype)

        h, rt_all = pl.pallas_call(
            functools.partial(expert_in, side, slots, chunks),
            out_shape=(
                jax.ShapeDtypeStruct((experts, members * slots, ff), BF16),
                jax.ShapeDtypeStruct((2, side, 2 * top, tokens), F32),
            ),
            in_specs=[vmem, vmem, anywhere, anywhere],
            out_specs=(anywhere, vmem),
            scratch_shapes=[
                buf(2, side, 2 * top, tokens, dtype=F32),
                buf(2, chunks, 3, tokens, HALF),
                buf(2, chunks, 2, 2, rows, HALF),
                buf(2, 3, side, rows, HALF),
                buf(2, chunks, side, side, rows, HALF),
                buf(2, side, side, rows, tokens),
                buf(3, wide, part),
                buf(3, wide, part),
                buf(experts, members * slots, ff, dtype=F32),
                buf(experts, members * slots, ff, dtype=F32),
                buf(members * slots, wide),
                buf(2, members * slots, part),
                dma((2, side)),
                dma((2, side)),
                dma((10, 2, chunks)),
                dma((10, 2, chunks)),
                dma((2, 3)),
                dma((2,)),
            ],
            compiler_params=pltpu.CompilerParams(collective_id=0, has_side_effects=True, vmem_limit_bytes=VMEM_BYTES),
            name="expert_in",
        )(rt, x, w_gate, w_up)

        y = pl.pallas_call(
            functools.partial(expert_out, side, slots, chunks),
            out_shape=jax.ShapeDtypeStruct((tokens, d), BF16),
            in_specs=[vmem, vmem] + [anywhere] * 5,
            out_specs=vmem,
            scratch_shapes=[
                buf(experts, members * slots, ff),
                buf(2, ff, wide),
                buf(2, 2, side, side, rows, HALF),
                buf(2, chunks, 3, side, rows, HALF),
                buf(2, chunks, 2, 2, rows, HALF),
                buf(2, side, side, tokens, rows),
                buf(2, 2, tokens, HALF, dtype=F32),
                buf(2, 2, tokens // 2, HALF),
                buf(2, chunks, 2, tokens // 2, HALF),
                buf(2, 2, tokens, HALF),
                buf(2, chunks, 2, tokens, HALF),
                buf(tokens, d, dtype=F32),
                buf(2, d, 256),
                buf(2, d, 256),
                buf(2, ff, wide),
                buf(tokens, ff),
                dma((10, 2, chunks)),
                dma((10, 2, chunks)),
                dma((2,)),
                dma((experts,)),
                dma((3, 2)),
            ],
            compiler_params=pltpu.CompilerParams(collective_id=1, has_side_effects=True, vmem_limit_bytes=VMEM_BYTES),
            name="expert_out",
        )(rt_all, x, h, w_down, s_gate, s_up, s_down)
        return y[None, None]

    tok = P("dp", "ep", None, None)
    return jax.shard_map(
        local,
        mesh=mesh,
        in_specs=(tok, tok, tok, tok, P("ep"), P("ep"), P("ep"), P(), P(), P()),
        out_specs=tok,
        check_vma=False,
    )
```

```python
import functools
import math

import jax
import jax.numpy as jnp
from jax import lax
from jax.experimental import pallas as pl
from jax.experimental.pallas import tpu as pltpu
from jax.sharding import PartitionSpec as P

MESH = pl.DeviceIdType.MESH
F32, BF16 = jnp.float32, jnp.bfloat16
VMEM_BYTES = 67_000_000
HALF = 256


def dot(a, b):
    return jnp.dot(a, b, preferred_element_type=F32)


class Place:
    def __init__(self, side):
        me = lax.axis_index("ep")
        self.side, self.x, self.y = side, me // side, me % side

    def at(self, dx, dy):
        s = self.side
        return (self.x + (dx % s)) % s * s + (self.y + (dy % s)) % s

    def first(self, half, d):
        return self.at(d, 0) if half == 0 else self.at(0, d)

    def both(self, half, first, second):
        return self.at(first, second) if half == 0 else self.at(second, first)

    def second(self, half, d):
        return self.at(0, d) if half == 0 else self.at(d, 0)


def turn(r):
    return 1 if r < 2 else -1


def pairs(place, half, i, r):
    j = (0, -turn(r), 0, turn(r))[i]
    return (0 if i < 2 else 1, r), place.second(half, j)


def hits(rt, base, rows, tokens, weighted):
    row = lax.broadcasted_iota(jnp.int32, (rows, tokens), 0).astype(F32) + base.astype(F32)
    top = rt.shape[0] // 2
    total = jnp.zeros((rows, tokens), F32)
    for k in range(top):
        value = rt[top + k : top + k + 1, :] if weighted else jnp.ones((1, tokens), F32)
        total = total + jnp.where(rt[k : k + 1, :] == row, value, 0.0)
    return total


def expert_in(side, slots, chunks, rt_ref, x_ref, wg_hbm, wu_hbm, h_hbm, rt_out,
              rtb, raw, nraw, pk, fw, zl, zb, dm, wgb, wub, accg, accu, ze, hst,
              rs, rr, ps, pr, ws, hs):
    place = Place(side)
    tokens, rows = x_ref.shape[0], dm.shape[3] // 2
    experts, _, ff = accg.shape
    wide = 2 * HALF
    part = wgb.shape[2]
    parts = ff // part
    steps = chunks * experts * parts

    barrier = pltpu.get_barrier_semaphore()
    for dx in range(side):
        for dy in range(side):
            if (dx, dy) != (0, 0):
                pl.semaphore_signal(barrier, inc=1, device_id={"ep": place.at(dx, dy)}, device_id_type=MESH)

    def weights(step):
        slot = step % 3
        c, e, n = step // (experts * parts), step // parts % experts, step % parts
        at = (e, pl.ds(pl.multiple_of(c * wide, wide), wide), pl.ds(pl.multiple_of(n * part, part), part))
        return (
            pltpu.make_async_copy(wg_hbm.at[at], wgb.at[slot], ws.at[0, slot]),
            pltpu.make_async_copy(wu_hbm.at[at], wub.at[slot], ws.at[1, slot]),
        )

    for step in (0, 1):
        for copy in weights(step):
            copy.start()
    for half in (0, 1):
        rtb[half, 0, 0] = rt_ref[...]
    pl.semaphore_wait(barrier, side * side - 1)

    def routing(half, g, r):
        across = 0 if g == 0 else turn(r)
        return pltpu.make_async_remote_copy(
            src_ref=rt_ref, dst_ref=rtb.at[half, g, r], send_sem=rs.at[half, g, r], recv_sem=rr.at[half, g, r],
            device_id={"ep": place.both(half, -r, across)}, device_id_type=MESH)

    routes = [(half, g, r) for g in (0, 1) for half in (0, 1) for r in range(side) if (g, r) != (0, 0)]

    def cols(half, c):
        return pl.ds(pl.multiple_of(c * wide + half * HALF, HALF), HALF)

    low, high = pl.ds(0, tokens // 2), pl.ds(tokens // 2, tokens // 2)

    def send(kind, half, c):
        plus, minus = (1, -1)
        src, dst, to = [
            lambda: (x_ref.at[:, cols(half, c)], raw.at[half, c, 2], place.first(half, plus)),
            lambda: (x_ref.at[:, cols(half, c)], raw.at[half, c, 0], place.first(half, minus)),
            lambda: (raw.at[half, c, 2, low], raw.at[half, c, 1, low], place.first(half, plus)),
            lambda: (raw.at[half, c, 0, high], raw.at[half, c, 1, high], place.first(half, minus)),
            lambda: (x_ref.at[:, cols(half, c)], nraw.at[half, c, 0, 0], place.second(half, plus)),
            lambda: (raw.at[half, c, 0], nraw.at[half, c, 0, 1], place.second(half, plus)),
            lambda: (raw.at[half, c, 1], nraw.at[half, c, 1, 0], place.second(half, minus)),
            lambda: (raw.at[half, c, 2], nraw.at[half, c, 1, 1], place.second(half, minus)),
            lambda: (pk.at[half, pl.ds(0, 2)], zb.at[half, c, 0, pl.ds(0, 2)], place.second(half, minus)),
            lambda: (pk.at[half, pl.ds(2, 2)], zb.at[half, c, 2, pl.ds(2, 2)], place.second(half, plus)),
            lambda: (fw.at[half, pl.ds(0, 2)], zb.at[half, c, 1, pl.ds(0, 2)], place.second(half, plus)),
            lambda: (fw.at[half, pl.ds(2, 2)], zb.at[half, c, 1, pl.ds(2, 2)], place.second(half, minus)),
        ][kind]()
        return pltpu.make_async_remote_copy(
            src_ref=src, dst_ref=dst, send_sem=ps.at[kind, half, c], recv_sem=pr.at[kind, half, c],
            device_id={"ep": to}, device_id_type=MESH)

    def own_blocks(c):
        for half in (0, 1):
            send(0, half, c).start()
            send(1, half, c).start()
        for half in (0, 1):
            send(4, half, c).start()

    def pass_blocks(c):
        for half in (0, 1):
            send(0, half, c).wait_recv()
            send(2, half, c).start()
            send(1, half, c).wait_recv()
            send(3, half, c).start()
        for half in (0, 1):
            send(7, half, c).start()
            send(5, half, c).start()

    def pick(half, stage, r, block):
        out = dot(dm[half, stage, r], block).astype(BF16)
        return out[:rows], out[rows:]

    def block(half, c, r):
        return x_ref[:, cols(half, c)] if r == 0 else raw[half, c, r - 1]

    def relay(half, c):
        @pl.when(c > 0)
        def _():
            for kind in (8, 9):
                send(kind, half, c - 1).wait_send()

        send(2, half, c).wait_recv()
        send(3, half, c).wait_recv()
        send(6, half, c).start()
        for r in range(side):
            pk[half, r], zl[half, c % 3, r] = pick(half, 0, r, block(half, c, r))
            if r >= 2:
                send(6 + r, half, c).start()

    def pass_rows(half, c):
        @pl.when(c > 0)
        def _():
            for kind in (10, 11):
                send(kind, half, c - 1).wait_send()

        for kind in (4, 5, 6, 7):
            send(kind, half, c).wait_recv()
        for r in range(side):
            fw[half, r], zb[half, c, 2 if r < 2 else 0, r] = pick(half, 1, r, nraw[half, c, r // 2, r % 2])
            if r >= 2:
                send(8 + r, half, c).start()

    def arrive(c):
        for half in (0, 1):
            for kind in (8, 9, 10, 11):
                send(kind, half, c).wait_recv()

    def compute(c, first, end, last):
        def expert(e, carry):
            mine = pl.ds(pl.multiple_of(e * slots, slots), slots)
            for dx in range(side):
                for dy in range(side):
                    at = pl.ds((dx * side + dy) * slots, slots)
                    ze[at, 0:HALF] = zl[0, c % 3, dx, mine, :] if dy == 0 else zb[0, c, dy - 1, dx, mine, :]
                    ze[at, HALF:wide] = zl[1, c % 3, dy, mine, :] if dx == 0 else zb[1, c, dx - 1, dy, mine, :]

            def columns(n, carry):
                step = (c * experts + e) * parts + n

                @pl.when(step + 2 < steps)
                def _():
                    for copy in weights(step + 2):
                        copy.start()

                for copy in weights(step):
                    copy.wait()
                slot = step % 3
                if last:

                    @pl.when(e > 0)
                    def _():
                        result(e - 1, n).wait()

                for t in range(part // 256):
                    at = pl.ds(t * 256, 256)
                    to = pl.ds(pl.multiple_of(n * part + t * 256, 256), 256)
                    g = accg[e, :, to] + dot(ze[...], wgb[slot, :, at])
                    u = accu[e, :, to] + dot(ze[...], wub[slot, :, at])
                    if last:
                        hst[n, :, at] = (jax.nn.silu(g) * u).astype(BF16)
                    else:
                        accg[e, :, to] = g
                        accu[e, :, to] = u
                if last:
                    result(e, n).start()
                return carry

            return lax.fori_loop(0, parts, columns, carry)

        lax.fori_loop(first, end, expert, 0)

    def result(e, n):
        return pltpu.make_async_copy(hst.at[n], h_hbm.at[e, :, pl.ds(pl.multiple_of(n * part, part), part)], hs.at[n])

    own_blocks(0)
    for route in routes:
        routing(*route).start()
    own_blocks(1)

    def clear(i, carry):
        at = pl.ds(pl.multiple_of(i * 128, 128), 128)
        for e in range(experts):
            accg[e, :, at] = jnp.zeros((accg.shape[1], 128), F32)
            accu[e, :, at] = jnp.zeros((accg.shape[1], 128), F32)
        return carry

    pass_blocks(0)
    lax.fori_loop(0, ff // 128, clear, 0)
    for half in (0, 1):
        for r in range(1, side):
            routing(half, 0, r).wait_recv()

    def select(half, stage):
        for r in range(side):
            for n in (0, 1):
                (g, at), device = pairs(place, half, 2 * stage + 1 - n, r)
                dm[half, stage, r, n * rows : (n + 1) * rows] = hits(
                    rtb[half, g, at], device * rows, rows, tokens, False).astype(BF16)

    for half in (0, 1):
        select(half, 0)
        relay(half, 0)
    pass_blocks(1)
    own_blocks(2)

    for half in (0, 1):
        for r in range(side):
            routing(half, 1, r).wait_recv()
        select(half, 1)

    def chunk(c, carry):
        pass_rows(0, c)
        pass_rows(1, c)

        @pl.when(c + 1 < chunks)
        def _():
            relay(0, c + 1)

        @pl.when(c > 0)
        def _():
            arrive(c - 1)
            compute(c - 1, 0, 2, False)

        @pl.when(c + 1 < chunks)
        def _():
            relay(1, c + 1)

        @pl.when(c > 0)
        def _():
            compute(c - 1, 2, 3, False)

        @pl.when(c + 2 < chunks)
        def _():
            pass_blocks(c + 2)

        @pl.when(c > 0)
        def _():
            compute(c - 1, 3, experts, False)

        @pl.when(c + 3 < chunks)
        def _():
            own_blocks(c + 3)

        return carry

    lax.fori_loop(0, chunks, chunk, 0)
    arrive(chunks - 1)
    compute(chunks - 1, 0, experts, True)
    for n in range(parts):
        result(experts - 1, n).wait()
    rt_out[...] = rtb[...]

    def drain(c, carry):
        for half in (0, 1):
            for kind in range(8):
                send(kind, half, c).wait_send()
        return carry

    lax.fori_loop(0, chunks, drain, 0)
    for half in (0, 1):
        for kind in (8, 9, 10, 11):
            send(kind, half, chunks - 1).wait_send()
    for route in routes:
        routing(*route).wait_send()


def expert_out(side, slots, chunks, rt_ref, x_ref, h_hbm, wd_hbm, sg_hbm, su_hbm, sd_hbm, y_ref,
               hb, wdb, ob, rb, tran, tb, tokb, cm, summed, hs, hr, ss, sr, yacc, sgb, sub, sdb, hsb,
               ps, pr, ws, hsem, ssem):
    place = Place(side)
    tokens = x_ref.shape[0]
    rows = ob.shape[4]
    experts = hb.shape[0]
    ff = hsb.shape[1]
    wide = 2 * HALF
    steps = chunks * experts
    half_rows = tokens // 2
    low, high = pl.ds(0, half_rows), pl.ds(half_rows, half_rows)

    barrier = pltpu.get_barrier_semaphore()
    for half in (0, 1):
        for d in (1, -1):
            pl.semaphore_signal(barrier, inc=1, device_id={"ep": place.first(half, d)}, device_id_type=MESH)

    def load_h(e):
        return pltpu.make_async_copy(h_hbm.at[e], hb.at[e], hsem.at[e])

    def weights(step):
        slot = step % 2
        c, e = step // experts, step % experts
        return pltpu.make_async_copy(
            wd_hbm.at[e, :, pl.ds(pl.multiple_of(c * wide, wide), wide)], wdb.at[slot], ws.at[slot])

    load_h(0).start()
    weights(0).start()
    for e in range(1, experts):
        load_h(e).start()

    def send(kind, half, c):
        plus, minus = (1, -1)
        par = c % 3
        src, dst, to = [
            lambda: (ob.at[half, par, 2, pl.ds(0, 2)], tran.at[half, c, 0], place.second(half, minus)),
            lambda: (ob.at[half, par, 2, pl.ds(2, 2)], tran.at[half, c, 1], place.second(half, plus)),
            lambda: (ob.at[half, par, 1, pl.ds(0, 2)], rb.at[half, c, 0], place.second(half, plus)),
            lambda: (ob.at[half, par, 3, pl.ds(2, 2)], rb.at[half, c, 1], place.second(half, minus)),
            lambda: (tokb.at[half, 0], tb.at[half, c, 0], place.second(half, minus)),
            lambda: (tokb.at[half, 1], tb.at[half, c, 1], place.second(half, plus)),
            lambda: (hs.at[half, 0], hr.at[half, c, 0], place.first(half, plus)),
            lambda: (hs.at[half, 1], hr.at[half, c, 1], place.first(half, minus)),
            lambda: (ss.at[half, 0], sr.at[half, c, 0], place.first(half, plus)),
            lambda: (ss.at[half, 1], sr.at[half, c, 1], place.first(half, minus)),
        ][kind]()
        return pltpu.make_async_remote_copy(
            src_ref=src, dst_ref=dst, send_sem=ps.at[kind, half, c], recv_sem=pr.at[kind, half, c],
            device_id={"ep": to}, device_id_type=MESH)

    def down(c, loading=False):
        par = c % 3

        def expert(e, carry):
            step = c * experts + e

            @pl.when(step + 1 < steps)
            def _():
                weights(step + 1).start()

            weights(step).wait()
            if loading:
                load_h(e).wait()
            mine = pl.ds(pl.multiple_of(e * slots, slots), slots)
            for half in (0, 1):
                out = dot(hb[e], wdb[step % 2, :, half * HALF : (half + 1) * HALF]).astype(BF16)
                for dx in range(side):
                    for dy in range(side):
                        j, r = (dy, dx) if half == 0 else (dx, dy)
                        at = (dx * side + dy) * slots
                        ob[half, par, j, r, mine, :] = out[at : at + slots]
            return carry

        lax.fori_loop(0, experts, expert, 0)

    def send_rows(c):
        for half in (0, 1):
            for kind in (0, 1, 2, 3):
                send(kind, half, c).start()

    def pass_rows(c):
        par = c % 3
        for half in (0, 1):

            @pl.when(c > 0)
            def _():
                for kind in (4, 5):
                    send(kind, half, c - 1).wait_send()

            for way in (0, 1):
                send(way, half, c).wait_recv()
                for n in range(2):
                    r = 2 * way + n
                    total = dot(cm[half, 2, r], ob[half, par, 3 if way == 0 else 1, r])
                    tokb[half, way, n] = (total + dot(cm[half, 3, r], tran[half, c, way, n])).astype(BF16)
            for way in (0, 1):
                send(way + 4, half, c).start()

    def relay(c):
        par = c % 3
        for half in (0, 1):
            for kind in (2, 3, 4, 5):
                send(kind, half, c).wait_recv()

            def total(r):
                out = dot(cm[half, 0, r], ob[half, par, 0, r]) + dot(cm[half, 1, r], rb[half, c, r // 2, r % 2])
                return out + tb[half, c, r // 2, r % 2].astype(F32)

            far = total(2).astype(BF16)

            @pl.when(c > 0)
            def _():
                for kind in (6, 7):
                    send(kind, half, c - 1).wait_send()

            hs[half, 0] = far[:half_rows]
            hs[half, 1] = far[half_rows:]
            summed[half, 0] = total(1)
            send(6, half, c).start()
            summed[half, 1] = total(3)
            send(7, half, c).start()
            at = pl.ds(pl.multiple_of(c * wide + half * HALF, HALF), HALF)
            yacc[:, at] += total(0)

    def near(c):
        for half in (0, 1):

            @pl.when(c > 0)
            def _():
                for kind in (8, 9):
                    send(kind, half, c - 1).wait_send()

            send(6, half, c).wait_recv()
            ss[half, 0, low] = (summed[half, 0, low] + hr[half, c, 0].astype(F32)).astype(BF16)
            ss[half, 0, high] = summed[half, 0, high].astype(BF16)
            send(7, half, c).wait_recv()
            ss[half, 1, low] = summed[half, 1, low].astype(BF16)
            ss[half, 1, high] = (summed[half, 1, high] + hr[half, c, 1].astype(F32)).astype(BF16)
            send(8, half, c).start()
            send(9, half, c).start()

    def finish(c):
        for half in (0, 1):
            for kind in (8, 9):
                send(kind, half, c).wait_recv()
            at = pl.ds(pl.multiple_of(c * wide + half * HALF, HALF), HALF)
            total = yacc[:, at] + sr[half, c, 0].astype(F32) + sr[half, c, 1].astype(F32)
            y_ref[:, at] = total.astype(BF16)

    def shared_in(n):
        at = pl.ds(pl.multiple_of(n * 256, 256), 256)
        return (
            pltpu.make_async_copy(sg_hbm.at[:, at], sgb.at[n % 2], ssem.at[0, n % 2]),
            pltpu.make_async_copy(su_hbm.at[:, at], sub.at[n % 2], ssem.at[1, n % 2]),
        )

    def shared_out(n):
        at = pl.ds(pl.multiple_of(n * wide, wide), wide)
        return pltpu.make_async_copy(sd_hbm.at[:, at], sdb.at[n % 2], ssem.at[2, n % 2])

    def inner(n):
        @pl.when(n + 1 < ff // 256)
        def _():
            for copy in shared_in(n + 1):
                copy.start()

        for copy in shared_in(n):
            copy.wait()
        g = dot(x_ref[...], sgb[n % 2])
        u = dot(x_ref[...], sub[n % 2])
        hsb[:, pl.ds(pl.multiple_of(n * 256, 256), 256)] = (jax.nn.silu(g) * u).astype(BF16)

    def outer(n):
        @pl.when(n + 1 < chunks)
        def _():
            shared_out(n + 1).start()

        shared_out(n).wait()
        yacc[:, pl.ds(pl.multiple_of(n * wide, wide), wide)] += dot(hsb[...], sdb[n % 2])

    pieces = ff // 256 + chunks
    per = -(-pieces // (chunks - 1))

    def shared(c):
        def piece(p, carry):
            @pl.when(p < ff // 256)
            def _():
                inner(p)

            @pl.when((p >= ff // 256) & (p < pieces))
            def _():
                outer(p - ff // 256)

            return carry

        lax.fori_loop(c * per, c * per + per, piece, 0)

    down(0, True)
    pl.semaphore_wait(barrier, 4)
    send_rows(0)
    for copy in shared_in(0):
        copy.start()
    shared_out(0).start()
    down(1)
    send_rows(1)

    def select(some):
        for half in (0, 1):
            for i in some:
                for r in range(side):
                    (g, at), device = pairs(place, half, i, r)
                    cm[half, i, r] = hits(rt_ref[half, g, at], device * rows, rows, tokens, True).T.astype(BF16)

    select((2, 3))
    pass_rows(0)
    down(2)
    send_rows(2)
    select((0, 1))
    yacc[...] = jnp.zeros(yacc.shape, F32)

    def chunk(c, carry):
        @pl.when(c > 0)
        def _():
            near(c - 1)

        relay(c)

        @pl.when(c + 1 < chunks)
        def _():
            pass_rows(c + 1)

        @pl.when(c + 3 < chunks)
        def _():
            for half in (0, 1):
                for kind in (0, 1, 2, 3):
                    send(kind, half, c).wait_send()
            down(c + 3)
            send_rows(c + 3)

        @pl.when(c + 1 < chunks)
        def _():
            shared(c)

        return carry

    lax.fori_loop(0, chunks, chunk, 0)
    near(chunks - 1)

    def end(c, carry):
        finish(c)
        return carry

    lax.fori_loop(0, chunks, end, 0)

    for half in (0, 1):
        for kind in (4, 5, 6, 7, 8, 9):
            send(kind, half, chunks - 1).wait_send()
        for c in (chunks - 3, chunks - 2, chunks - 1):
            for kind in (0, 1, 2, 3):
                send(kind, half, c).wait_send()


def solution(mesh):
    members = mesh.shape["ep"]
    side = math.isqrt(members)

    def local(x, expert, slot, gate, w_gate, w_up, w_down, s_gate, s_up, s_down):
        x, expert, slot, gate = x[0, 0], expert[0, 0], slot[0, 0], gate[0, 0]
        (tokens, top), (experts, d, ff) = expert.shape, w_gate.shape
        slots = 5 * tokens * top // (4 * experts * members)
        rows, wide = experts * slots, 2 * HALF
        chunks = d // wide
        part = ff // 2
        key = jnp.where(slot < slots, expert * slots + slot, -1).astype(F32)
        weight = gate.astype(BF16).astype(F32)
        rt = jnp.concatenate([key.T, weight.T], axis=0)

        vmem, anywhere = pl.BlockSpec(memory_space=pltpu.VMEM), pl.BlockSpec(memory_space=pl.ANY)
        dma = pltpu.SemaphoreType.DMA

        def buf(*shape, dtype=BF16):
            return pltpu.VMEM(shape, dtype)

        h, rt_all = pl.pallas_call(
            functools.partial(expert_in, side, slots, chunks),
            out_shape=(
                jax.ShapeDtypeStruct((experts, members * slots, ff), BF16),
                jax.ShapeDtypeStruct((2, 2, side, 2 * top, tokens), F32),
            ),
            in_specs=[vmem, vmem, anywhere, anywhere],
            out_specs=(anywhere, vmem),
            scratch_shapes=[
                buf(2, 2, side, 2 * top, tokens, dtype=F32),
                buf(2, chunks, 3, tokens, HALF),
                buf(2, chunks, 2, 2, tokens, HALF),
                buf(2, side, rows, HALF),
                buf(2, side, rows, HALF),
                buf(2, 3, side, rows, HALF),
                buf(2, chunks, side - 1, side, rows, HALF),
                buf(2, 2, side, 2 * rows, tokens),
                buf(3, wide, part),
                buf(3, wide, part),
                buf(experts, members * slots, ff, dtype=F32),
                buf(experts, members * slots, ff, dtype=F32),
                buf(members * slots, wide),
                buf(2, members * slots, part),
                dma((2, 2, side)),
                dma((2, 2, side)),
                dma((12, 2, chunks)),
                dma((12, 2, chunks)),
                dma((2, 3)),
                dma((2,)),
            ],
            compiler_params=pltpu.CompilerParams(collective_id=0, has_side_effects=True, vmem_limit_bytes=VMEM_BYTES),
            name="expert_in",
        )(rt, x, w_gate, w_up)

        y = pl.pallas_call(
            functools.partial(expert_out, side, slots, chunks),
            out_shape=jax.ShapeDtypeStruct((tokens, d), BF16),
            in_specs=[vmem, vmem] + [anywhere] * 5,
            out_specs=vmem,
            scratch_shapes=[
                buf(experts, members * slots, ff),
                buf(2, ff, wide),
                buf(2, 3, side, side, rows, HALF),
                buf(2, chunks, 2, 2, rows, HALF),
                buf(2, chunks, 2, 2, rows, HALF),
                buf(2, chunks, 2, 2, tokens, HALF),
                buf(2, 2, 2, tokens, HALF),
                buf(2, side, side, tokens, rows),
                buf(2, 2, tokens, HALF, dtype=F32),
                buf(2, 2, tokens // 2, HALF),
                buf(2, chunks, 2, tokens // 2, HALF),
                buf(2, 2, tokens, HALF),
                buf(2, chunks, 2, tokens, HALF),
                buf(tokens, d, dtype=F32),
                buf(2, d, 256),
                buf(2, d, 256),
                buf(2, ff, wide),
                buf(tokens, ff),
                dma((10, 2, chunks)),
                dma((10, 2, chunks)),
                dma((2,)),
                dma((experts,)),
                dma((3, 2)),
            ],
            compiler_params=pltpu.CompilerParams(collective_id=1, has_side_effects=True, vmem_limit_bytes=VMEM_BYTES),
            name="expert_out",
        )(rt_all, x, h, w_down, s_gate, s_up, s_down)
        return y[None, None]

    tok = P("dp", "ep", None, None)
    return jax.shard_map(
        local,
        mesh=mesh,
        in_specs=(tok, tok, tok, tok, P("ep"), P("ep"), P("ep"), P(), P(), P()),
        out_specs=tok,
        check_vma=False,
    )
```

```python
import functools
import math

import jax
import jax.numpy as jnp
from jax import lax
from jax.experimental import pallas as pl
from jax.experimental.pallas import tpu as pltpu
from jax.sharding import PartitionSpec as P

MESH = pl.DeviceIdType.MESH
F32, BF16 = jnp.float32, jnp.bfloat16
VMEM_BYTES = 67_000_000
HALF = 256
BOTH = (0, 1)
FRONT, BACK = pl.ds(0, 2), pl.ds(2, 2)
PLUS, MINUS = 1, -1


def dot(a, b):
    return jnp.dot(a, b, preferred_element_type=F32)


class Place:
    def __init__(self, side):
        me = lax.axis_index("ep")
        self.side, self.x, self.y = side, me // side, me % side

    def at(self, dx, dy):
        s = self.side
        return (self.x + (dx % s)) % s * s + (self.y + (dy % s)) % s

    def first(self, half, d):
        return self.at(d, 0) if half == 0 else self.at(0, d)

    def both(self, half, first, second):
        return self.at(first, second) if half == 0 else self.at(second, first)

    def second(self, half, d):
        return self.at(0, d) if half == 0 else self.at(d, 0)


def turn(r):
    return 1 if r < 2 else -1


def pairs(place, half, i, r):
    j = (0, -turn(r), 0, turn(r))[i]
    return (0 if i < 2 else 1, r), place.second(half, j)


def hits(rt, base, rows, tokens, weighted):
    row = lax.broadcasted_iota(jnp.int32, (rows, tokens), 0).astype(F32) + base.astype(F32)
    top = rt.shape[0] // 2
    total = jnp.zeros((rows, tokens), F32)
    for k in range(top):
        value = rt[top + k : top + k + 1, :] if weighted else jnp.ones((1, tokens), F32)
        total = total + jnp.where(rt[k : k + 1, :] == row, value, 0.0)
    return total


def expert_in(side, slots, chunks, rt_ref, x_ref, wg_hbm, wu_hbm, h_hbm, rt_out,
              rtb, raw, nraw, pk, fw, zl, zb, dm, wgb, wub, accg, accu, ze, hst,
              rs, rr, ps, pr, ws, hs):
    place = Place(side)
    tokens, rows = x_ref.shape[0], dm.shape[3] // 2
    experts, _, ff = accg.shape
    wide = 2 * HALF
    part = wgb.shape[2]
    parts = ff // part
    steps = chunks * experts * parts

    barrier = pltpu.get_barrier_semaphore()
    for dx in range(side):
        for dy in range(side):
            if (dx, dy) != (0, 0):
                pl.semaphore_signal(barrier, inc=1, device_id={"ep": place.at(dx, dy)}, device_id_type=MESH)

    def weights(step):
        slot = step % 3
        c, e, n = step // (experts * parts), step // parts % experts, step % parts
        at = (e, pl.ds(pl.multiple_of(c * wide, wide), wide), pl.ds(pl.multiple_of(n * part, part), part))
        return (
            pltpu.make_async_copy(wg_hbm.at[at], wgb.at[slot], ws.at[0, slot]),
            pltpu.make_async_copy(wu_hbm.at[at], wub.at[slot], ws.at[1, slot]),
        )

    for step in BOTH:
        for copy in weights(step):
            copy.start()
    for half in BOTH:
        rtb[half, 0, 0] = rt_ref[...]
    pl.semaphore_wait(barrier, side * side - 1)

    def routing(half, g, r):
        across = 0 if g == 0 else turn(r)
        return pltpu.make_async_remote_copy(
            src_ref=rt_ref, dst_ref=rtb.at[half, g, r], send_sem=rs.at[half, g, r], recv_sem=rr.at[half, g, r],
            device_id={"ep": place.both(half, -r, across)}, device_id_type=MESH)

    routes = [(half, g, r) for g in BOTH for half in BOTH for r in range(side) if (g, r) != (0, 0)]

    def cols(half, c):
        return pl.ds(pl.multiple_of(c * wide + half * HALF, HALF), HALF)

    low, high = pl.ds(0, tokens // 2), pl.ds(tokens // 2, tokens // 2)

    def send(kind, half, c):
        src, dst, to = [
            lambda: (x_ref.at[:, cols(half, c)], raw.at[half, c, 2], place.first(half, PLUS)),
            lambda: (x_ref.at[:, cols(half, c)], raw.at[half, c, 0], place.first(half, MINUS)),
            lambda: (raw.at[half, c, 2, low], raw.at[half, c, 1, low], place.first(half, PLUS)),
            lambda: (raw.at[half, c, 0, high], raw.at[half, c, 1, high], place.first(half, MINUS)),
            lambda: (x_ref.at[:, cols(half, c)], nraw.at[half, c, 0, 0], place.second(half, PLUS)),
            lambda: (raw.at[half, c, 0], nraw.at[half, c, 0, 1], place.second(half, PLUS)),
            lambda: (raw.at[half, c, 1], nraw.at[half, c, 1, 0], place.second(half, MINUS)),
            lambda: (raw.at[half, c, 2], nraw.at[half, c, 1, 1], place.second(half, MINUS)),
            lambda: (pk.at[half, FRONT], zb.at[half, c, 0, FRONT], place.second(half, MINUS)),
            lambda: (pk.at[half, BACK], zb.at[half, c, 2, BACK], place.second(half, PLUS)),
            lambda: (fw.at[half, FRONT], zb.at[half, c, 1, FRONT], place.second(half, PLUS)),
            lambda: (fw.at[half, BACK], zb.at[half, c, 1, BACK], place.second(half, MINUS)),
        ][kind]()
        return pltpu.make_async_remote_copy(
            src_ref=src, dst_ref=dst, send_sem=ps.at[kind, half, c], recv_sem=pr.at[kind, half, c],
            device_id={"ep": to}, device_id_type=MESH)

    def own_blocks(c):
        for half in BOTH:
            send(0, half, c).start()
            send(1, half, c).start()
        for half in BOTH:
            send(4, half, c).start()

    def pass_blocks(c):
        for half in BOTH:
            send(0, half, c).wait_recv()
            send(2, half, c).start()
            send(1, half, c).wait_recv()
            send(3, half, c).start()
        for half in BOTH:
            send(7, half, c).start()
            send(5, half, c).start()

    def pick(half, stage, r, block):
        out = dot(dm[half, stage, r], block).astype(BF16)
        return out[:rows], out[rows:]

    def block(half, c, r):
        return x_ref[:, cols(half, c)] if r == 0 else raw[half, c, r - 1]

    def relay(half, c):
        @pl.when(c > 0)
        def _():
            for kind in (8, 9):
                send(kind, half, c - 1).wait_send()

        send(2, half, c).wait_recv()
        send(3, half, c).wait_recv()
        send(6, half, c).start()
        for r in range(side):
            pk[half, r], zl[half, c % 3, r] = pick(half, 0, r, block(half, c, r))
            if r >= 2:
                send(6 + r, half, c).start()

    def pass_rows(half, c):
        @pl.when(c > 0)
        def _():
            for kind in (10, 11):
                send(kind, half, c - 1).wait_send()

        for kind in (4, 5, 6, 7):
            send(kind, half, c).wait_recv()
        for r in range(side):
            fw[half, r], zb[half, c, 2 if r < 2 else 0, r] = pick(half, 1, r, nraw[half, c, r // 2, r % 2])
            if r >= 2:
                send(8 + r, half, c).start()

    def arrive(c):
        for half in BOTH:
            for kind in (8, 9, 10, 11):
                send(kind, half, c).wait_recv()

    def compute(c, first, end, last):
        def expert(e, carry):
            mine = pl.ds(pl.multiple_of(e * slots, slots), slots)
            for dx in range(side):
                for dy in range(side):
                    at = pl.ds((dx * side + dy) * slots, slots)
                    ze[at, 0:HALF] = zl[0, c % 3, dx, mine, :] if dy == 0 else zb[0, c, dy - 1, dx, mine, :]
                    ze[at, HALF:wide] = zl[1, c % 3, dy, mine, :] if dx == 0 else zb[1, c, dx - 1, dy, mine, :]

            def columns(n, carry):
                step = (c * experts + e) * parts + n

                @pl.when(step + 2 < steps)
                def _():
                    for copy in weights(step + 2):
                        copy.start()

                for copy in weights(step):
                    copy.wait()
                slot = step % 3
                if last:

                    @pl.when(e > 0)
                    def _():
                        result(e - 1, n).wait()

                for t in range(part // 256):
                    at = pl.ds(t * 256, 256)
                    to = pl.ds(pl.multiple_of(n * part + t * 256, 256), 256)
                    g = accg[e, :, to] + dot(ze[...], wgb[slot, :, at])
                    u = accu[e, :, to] + dot(ze[...], wub[slot, :, at])
                    if last:
                        hst[n, :, at] = (jax.nn.silu(g) * u).astype(BF16)
                    else:
                        accg[e, :, to] = g
                        accu[e, :, to] = u
                if last:
                    result(e, n).start()
                return carry

            return lax.fori_loop(0, parts, columns, carry)

        lax.fori_loop(first, end, expert, 0)

    def result(e, n):
        return pltpu.make_async_copy(hst.at[n], h_hbm.at[e, :, pl.ds(pl.multiple_of(n * part, part), part)], hs.at[n])

    own_blocks(0)
    for route in routes:
        routing(*route).start()
    own_blocks(1)

    def clear(i, carry):
        at = pl.ds(pl.multiple_of(i * 128, 128), 128)
        for e in range(experts):
            accg[e, :, at] = jnp.zeros((accg.shape[1], 128), F32)
            accu[e, :, at] = jnp.zeros((accg.shape[1], 128), F32)
        return carry

    pass_blocks(0)
    lax.fori_loop(0, ff // 128, clear, 0)
    for half in BOTH:
        for r in range(1, side):
            routing(half, 0, r).wait_recv()

    def select(half, stage):
        for r in range(side):
            for n in BOTH:
                (g, at), device = pairs(place, half, 2 * stage + 1 - n, r)
                dm[half, stage, r, n * rows : (n + 1) * rows] = hits(
                    rtb[half, g, at], device * rows, rows, tokens, False).astype(BF16)

    for half in BOTH:
        select(half, 0)
        relay(half, 0)
    pass_blocks(1)
    own_blocks(2)

    for half in BOTH:
        for r in range(side):
            routing(half, 1, r).wait_recv()
        select(half, 1)

    def chunk(c, carry):
        pass_rows(0, c)
        pass_rows(1, c)

        @pl.when(c + 1 < chunks)
        def _():
            relay(0, c + 1)

        @pl.when(c > 0)
        def _():
            arrive(c - 1)
            compute(c - 1, 0, 2, False)

        @pl.when(c + 1 < chunks)
        def _():
            relay(1, c + 1)

        @pl.when(c > 0)
        def _():
            compute(c - 1, 2, 3, False)

        @pl.when(c + 2 < chunks)
        def _():
            pass_blocks(c + 2)

        @pl.when(c > 0)
        def _():
            compute(c - 1, 3, experts, False)

        @pl.when(c + 3 < chunks)
        def _():
            own_blocks(c + 3)

        return carry

    lax.fori_loop(0, chunks, chunk, 0)
    arrive(chunks - 1)
    compute(chunks - 1, 0, experts, True)
    for n in range(parts):
        result(experts - 1, n).wait()
    rt_out[...] = rtb[...]

    def drain(c, carry):
        for half in BOTH:
            for kind in range(8):
                send(kind, half, c).wait_send()
        return carry

    lax.fori_loop(0, chunks, drain, 0)
    for half in BOTH:
        for kind in (8, 9, 10, 11):
            send(kind, half, chunks - 1).wait_send()
    for route in routes:
        routing(*route).wait_send()


def expert_out(side, slots, chunks, rt_ref, x_ref, h_hbm, wd_hbm, sg_hbm, su_hbm, sd_hbm, y_ref,
               hb, wdb, ob, rb, tran, tb, tokb, cm, summed, hs, hr, ss, sr, yacc, sgb, sub, sdb, hsb,
               ps, pr, ws, hsem, ssem):
    place = Place(side)
    tokens = x_ref.shape[0]
    rows = ob.shape[4]
    experts = hb.shape[0]
    ff = hsb.shape[1]
    wide = 2 * HALF
    steps = chunks * experts
    half_rows = tokens // 2
    low, high = pl.ds(0, half_rows), pl.ds(half_rows, half_rows)

    barrier = pltpu.get_barrier_semaphore()
    for half in BOTH:
        for d in (1, -1):
            pl.semaphore_signal(barrier, inc=1, device_id={"ep": place.first(half, d)}, device_id_type=MESH)

    def load_h(e):
        return pltpu.make_async_copy(h_hbm.at[e], hb.at[e], hsem.at[e])

    def weights(step):
        slot = step % 2
        c, e = step // experts, step % experts
        return pltpu.make_async_copy(
            wd_hbm.at[e, :, pl.ds(pl.multiple_of(c * wide, wide), wide)], wdb.at[slot], ws.at[slot])

    load_h(0).start()
    weights(0).start()
    for e in range(1, experts):
        load_h(e).start()

    def send(kind, half, c):
        par = c % 3
        src, dst, to = [
            lambda: (ob.at[half, par, 2, FRONT], tran.at[half, c, 0], place.second(half, MINUS)),
            lambda: (ob.at[half, par, 2, BACK], tran.at[half, c, 1], place.second(half, PLUS)),
            lambda: (ob.at[half, par, 1, FRONT], rb.at[half, c, 0], place.second(half, PLUS)),
            lambda: (ob.at[half, par, 3, BACK], rb.at[half, c, 1], place.second(half, MINUS)),
            lambda: (tokb.at[half, 0], tb.at[half, c, 0], place.second(half, MINUS)),
            lambda: (tokb.at[half, 1], tb.at[half, c, 1], place.second(half, PLUS)),
            lambda: (hs.at[half, 0], hr.at[half, c, 0], place.first(half, PLUS)),
            lambda: (hs.at[half, 1], hr.at[half, c, 1], place.first(half, MINUS)),
            lambda: (ss.at[half, 0], sr.at[half, c, 0], place.first(half, PLUS)),
            lambda: (ss.at[half, 1], sr.at[half, c, 1], place.first(half, MINUS)),
        ][kind]()
        return pltpu.make_async_remote_copy(
            src_ref=src, dst_ref=dst, send_sem=ps.at[kind, half, c], recv_sem=pr.at[kind, half, c],
            device_id={"ep": to}, device_id_type=MESH)

    def down(c, loading=False):
        par = c % 3

        def expert(e, carry):
            step = c * experts + e

            @pl.when(step + 1 < steps)
            def _():
                weights(step + 1).start()

            weights(step).wait()
            if loading:
                load_h(e).wait()
            mine = pl.ds(pl.multiple_of(e * slots, slots), slots)
            for half in BOTH:
                out = dot(hb[e], wdb[step % 2, :, half * HALF : (half + 1) * HALF]).astype(BF16)
                for dx in range(side):
                    for dy in range(side):
                        j, r = (dy, dx) if half == 0 else (dx, dy)
                        at = (dx * side + dy) * slots
                        ob[half, par, j, r, mine, :] = out[at : at + slots]
            return carry

        lax.fori_loop(0, experts, expert, 0)

    def send_rows(c):
        for half in BOTH:
            for kind in (0, 1, 2, 3):
                send(kind, half, c).start()

    def pass_rows(c):
        par = c % 3
        for half in BOTH:

            @pl.when(c > 0)
            def _():
                for kind in (4, 5):
                    send(kind, half, c - 1).wait_send()

            for way in BOTH:
                send(way, half, c).wait_recv()
                for n in range(2):
                    r = 2 * way + n
                    total = dot(cm[half, 2, r], ob[half, par, 3 if way == 0 else 1, r])
                    tokb[half, way, n] = (total + dot(cm[half, 3, r], tran[half, c, way, n])).astype(BF16)
            for way in BOTH:
                send(way + 4, half, c).start()

    def relay(c):
        par = c % 3
        for half in BOTH:
            for kind in (2, 3, 4, 5):
                send(kind, half, c).wait_recv()

            def total(r):
                out = dot(cm[half, 0, r], ob[half, par, 0, r]) + dot(cm[half, 1, r], rb[half, c, r // 2, r % 2])
                return out + tb[half, c, r // 2, r % 2].astype(F32)

            far = total(2).astype(BF16)

            @pl.when(c > 0)
            def _():
                for kind in (6, 7):
                    send(kind, half, c - 1).wait_send()

            hs[half, 0] = far[:half_rows]
            hs[half, 1] = far[half_rows:]
            summed[half, 0] = total(1)
            send(6, half, c).start()
            summed[half, 1] = total(3)
            send(7, half, c).start()
            at = pl.ds(pl.multiple_of(c * wide + half * HALF, HALF), HALF)
            yacc[:, at] += total(0)

    def near(c):
        for half in BOTH:

            @pl.when(c > 0)
            def _():
                for kind in (8, 9):
                    send(kind, half, c - 1).wait_send()

            send(6, half, c).wait_recv()
            ss[half, 0, low] = (summed[half, 0, low] + hr[half, c, 0].astype(F32)).astype(BF16)
            ss[half, 0, high] = summed[half, 0, high].astype(BF16)
            send(7, half, c).wait_recv()
            ss[half, 1, low] = summed[half, 1, low].astype(BF16)
            ss[half, 1, high] = (summed[half, 1, high] + hr[half, c, 1].astype(F32)).astype(BF16)
            send(8, half, c).start()
            send(9, half, c).start()

    def finish(c):
        for half in BOTH:
            for kind in (8, 9):
                send(kind, half, c).wait_recv()
            at = pl.ds(pl.multiple_of(c * wide + half * HALF, HALF), HALF)
            total = yacc[:, at] + sr[half, c, 0].astype(F32) + sr[half, c, 1].astype(F32)
            y_ref[:, at] = total.astype(BF16)

    def shared_in(n):
        at = pl.ds(pl.multiple_of(n * 256, 256), 256)
        return (
            pltpu.make_async_copy(sg_hbm.at[:, at], sgb.at[n % 2], ssem.at[0, n % 2]),
            pltpu.make_async_copy(su_hbm.at[:, at], sub.at[n % 2], ssem.at[1, n % 2]),
        )

    def shared_out(n):
        at = pl.ds(pl.multiple_of(n * wide, wide), wide)
        return pltpu.make_async_copy(sd_hbm.at[:, at], sdb.at[n % 2], ssem.at[2, n % 2])

    def inner(n):
        @pl.when(n + 1 < ff // 256)
        def _():
            for copy in shared_in(n + 1):
                copy.start()

        for copy in shared_in(n):
            copy.wait()
        g = dot(x_ref[...], sgb[n % 2])
        u = dot(x_ref[...], sub[n % 2])
        hsb[:, pl.ds(pl.multiple_of(n * 256, 256), 256)] = (jax.nn.silu(g) * u).astype(BF16)

    def outer(n):
        @pl.when(n + 1 < chunks)
        def _():
            shared_out(n + 1).start()

        shared_out(n).wait()
        yacc[:, pl.ds(pl.multiple_of(n * wide, wide), wide)] += dot(hsb[...], sdb[n % 2])

    pieces = ff // 256 + chunks
    per = -(-pieces // (chunks - 1))

    def shared(c):
        def piece(p, carry):
            @pl.when(p < ff // 256)
            def _():
                inner(p)

            @pl.when((p >= ff // 256) & (p < pieces))
            def _():
                outer(p - ff // 256)

            return carry

        lax.fori_loop(c * per, c * per + per, piece, 0)

    down(0, True)
    pl.semaphore_wait(barrier, 4)
    send_rows(0)
    for copy in shared_in(0):
        copy.start()
    shared_out(0).start()
    down(1)
    send_rows(1)

    def select(some):
        for half in BOTH:
            for i in some:
                for r in range(side):
                    (g, at), device = pairs(place, half, i, r)
                    cm[half, i, r] = hits(rt_ref[half, g, at], device * rows, rows, tokens, True).T.astype(BF16)

    select((2, 3))
    pass_rows(0)
    down(2)
    send_rows(2)
    select((0, 1))
    yacc[...] = jnp.zeros(yacc.shape, F32)

    def chunk(c, carry):
        @pl.when(c > 0)
        def _():
            near(c - 1)

        relay(c)

        @pl.when(c + 1 < chunks)
        def _():
            pass_rows(c + 1)

        @pl.when(c + 3 < chunks)
        def _():
            for half in BOTH:
                for kind in (0, 1, 2, 3):
                    send(kind, half, c).wait_send()
            down(c + 3)
            send_rows(c + 3)

        @pl.when(c + 1 < chunks)
        def _():
            shared(c)

        return carry

    lax.fori_loop(0, chunks, chunk, 0)
    near(chunks - 1)

    def end(c, carry):
        finish(c)
        return carry

    lax.fori_loop(0, chunks, end, 0)

    for half in BOTH:
        for kind in (4, 5, 6, 7, 8, 9):
            send(kind, half, chunks - 1).wait_send()
        for c in (chunks - 3, chunks - 2, chunks - 1):
            for kind in (0, 1, 2, 3):
                send(kind, half, c).wait_send()


def solution(mesh):
    members = mesh.shape["ep"]
    side = math.isqrt(members)

    def local(x, expert, slot, gate, w_gate, w_up, w_down, s_gate, s_up, s_down):
        x, expert, slot, gate = x[0, 0], expert[0, 0], slot[0, 0], gate[0, 0]
        (tokens, top), (experts, d, ff) = expert.shape, w_gate.shape
        slots = 5 * tokens * top // (4 * experts * members)
        rows, wide = experts * slots, 2 * HALF
        chunks = d // wide
        part = ff // 2
        key = jnp.where(slot < slots, expert * slots + slot, -1).astype(F32)
        weight = gate.astype(BF16).astype(F32)
        rt = jnp.concatenate([key.T, weight.T], axis=0)

        vmem, anywhere = pl.BlockSpec(memory_space=pltpu.VMEM), pl.BlockSpec(memory_space=pl.ANY)
        dma = pltpu.SemaphoreType.DMA

        def buf(*shape, dtype=BF16):
            return pltpu.VMEM(shape, dtype)

        h, rt_all = pl.pallas_call(
            functools.partial(expert_in, side, slots, chunks),
            out_shape=(
                jax.ShapeDtypeStruct((experts, members * slots, ff), BF16),
                jax.ShapeDtypeStruct((2, 2, side, 2 * top, tokens), F32),
            ),
            in_specs=[vmem, vmem, anywhere, anywhere],
            out_specs=(anywhere, vmem),
            scratch_shapes=[
                buf(2, 2, side, 2 * top, tokens, dtype=F32),
                buf(2, chunks, 3, tokens, HALF),
                buf(2, chunks, 2, 2, tokens, HALF),
                buf(2, side, rows, HALF),
                buf(2, side, rows, HALF),
                buf(2, 3, side, rows, HALF),
                buf(2, chunks, side - 1, side, rows, HALF),
                buf(2, 2, side, 2 * rows, tokens),
                buf(3, wide, part),
                buf(3, wide, part),
                buf(experts, members * slots, ff, dtype=F32),
                buf(experts, members * slots, ff, dtype=F32),
                buf(members * slots, wide),
                buf(2, members * slots, part),
                dma((2, 2, side)),
                dma((2, 2, side)),
                dma((12, 2, chunks)),
                dma((12, 2, chunks)),
                dma((2, 3)),
                dma((2,)),
            ],
            compiler_params=pltpu.CompilerParams(collective_id=0, has_side_effects=True, vmem_limit_bytes=VMEM_BYTES),
            name="expert_in",
        )(rt, x, w_gate, w_up)

        y = pl.pallas_call(
            functools.partial(expert_out, side, slots, chunks),
            out_shape=jax.ShapeDtypeStruct((tokens, d), BF16),
            in_specs=[vmem, vmem] + [anywhere] * 5,
            out_specs=vmem,
            scratch_shapes=[
                buf(experts, members * slots, ff),
                buf(2, ff, wide),
                buf(2, 3, side, side, rows, HALF),
                buf(2, chunks, 2, 2, rows, HALF),
                buf(2, chunks, 2, 2, rows, HALF),
                buf(2, chunks, 2, 2, tokens, HALF),
                buf(2, 2, 2, tokens, HALF),
                buf(2, side, side, tokens, rows),
                buf(2, 2, tokens, HALF, dtype=F32),
                buf(2, 2, tokens // 2, HALF),
                buf(2, chunks, 2, tokens // 2, HALF),
                buf(2, 2, tokens, HALF),
                buf(2, chunks, 2, tokens, HALF),
                buf(tokens, d, dtype=F32),
                buf(2, d, 256),
                buf(2, d, 256),
                buf(2, ff, wide),
                buf(tokens, ff),
                dma((10, 2, chunks)),
                dma((10, 2, chunks)),
                dma((2,)),
                dma((experts,)),
                dma((3, 2)),
            ],
            compiler_params=pltpu.CompilerParams(collective_id=1, has_side_effects=True, vmem_limit_bytes=VMEM_BYTES),
            name="expert_out",
        )(rt_all, x, h, w_down, s_gate, s_up, s_down)
        return y[None, None]

    tok = P("dp", "ep", None, None)
    return jax.shard_map(
        local,
        mesh=mesh,
        in_specs=(tok, tok, tok, tok, P("ep"), P("ep"), P("ep"), P(), P(), P()),
        out_specs=tok,
        check_vma=False,
    )
```
